32 devices in a mesh: space: 32 (over z, y, x, core).
Axes of the slice: x: 2, y: 2, z: 4, core: 2. Of those that a mesh axis runs over, the one named last changes fastest.
Arguments:
- coords: float32 [512, 3, 128], P('space'), may hold values from -3 to 3
- force: float32 [512, 3, 128], P('space'), may hold values from -12 to 12
- restraint: float32 [512, 128], P('space'), may hold values from 0.25 to 4
- neighbors: int32 [512, 32], P('space'), may hold values from 0 to 511, as said below
- mask: int32 [512, 32], P('space'), may hold values from 0 to 1, as said below
Outputs:
- solution_field: float32 [512, 3, 128], P('space')
- residual: float32 [512, 3, 128], P('space')
The draws below stay inside these ranges and needn't reach their ends.
Inputs may be any that keep to these rules, and one draw needn't show every extreme that they name: `neighbors`: for every block b, the live entries name distinct blocks c with |c - b| <= 15; b itself is always live; if b lists c live then c lists b live; entries with mask 0 name b itself. `mask`: marks the live entries of neighbors.
All inputs are finite; a program needn't handle non-finite values.
Results may differ from the reference program's by a relative error of at most 0.0003.
Values sent between devices are 32-bit elements; how exact they have to be, the bound alone decides.
No kernel may reach another device: no remote copies, remote signals or barrier semaphores. Data moves between devices by JAX's collectives and lax.ppermute only.
A program may use at most 64 MiB of HBM per device.

```python
import math
import jax
import jax.numpy as jnp
from jax import lax

BA = 128
NB = 32
BLK_DEV = 16
ITERS = 2
NBLK = 512


def neighbor_tables(key):
    window = min(BLK_DEV, (NB - 1) // 2)
    block_ids = jnp.arange(NBLK, dtype=jnp.int32)
    offsets = jnp.arange(2 * window + 1, dtype=jnp.int32) - window
    partner = block_ids[:, None] + offsets[None, :]
    inside = (partner >= 0) & (partner < NBLK)
    lower_id = jnp.clip(jnp.minimum(partner, block_ids[:, None]), 0, NBLK - 1)
    upper_id = jnp.clip(jnp.maximum(partner, block_ids[:, None]), 0, NBLK - 1)
    pair_code = lower_id * NBLK + upper_id
    link_key = jax.random.fold_in(key, 11)
    hashed = jax.vmap(jax.vmap(lambda code: jax.random.randint(jax.random.fold_in(link_key, code), (), 0, 5)))(pair_code)
    linked = inside & ((hashed < 4) | (partner == block_ids[:, None]))
    padding = NB - (2 * window + 1)
    partner_full = jnp.concatenate([partner, jnp.broadcast_to(block_ids[:, None], (NBLK, padding))], axis=1)
    linked_full = jnp.concatenate([linked, jnp.zeros((NBLK, padding), dtype=bool)], axis=1)
    scores = jax.random.randint(jax.random.fold_in(key, 12), (NBLK, NB), 0, 2 ** 20) * NB + jnp.arange(NB, dtype=jnp.int32)[None, :]
    ranking = jnp.argsort(scores, axis=1)
    partner_full = jnp.take_along_axis(partner_full, ranking, axis=1)
    linked_full = jnp.take_along_axis(linked_full, ranking, axis=1)
    chosen = jnp.where(linked_full, partner_full, block_ids[:, None]).astype(jnp.int32)
    return (chosen, linked_full.astype(jnp.int32))


def draw_neighbors(key, part):
    return neighbor_tables(key)[0]


def draw_mask(key, part):
    return neighbor_tables(key)[1]


def draw_force(key, part):
    rising = 3.0 ** (0.5 * jnp.arange(NBLK, dtype=jnp.float32) / (NBLK - 1))
    normal_part = jnp.clip(jax.random.normal(jax.random.fold_in(key, 23), (NBLK, 3, BA), jnp.float32), -4.0, 4.0)
    values = normal_part * rising[:, None, None]
    return values.astype(jnp.float32)


def steps_of(rng, dims, pieces, smallest, high):
    loudness, own = 1.0, jax.random.fold_in(rng, 6)
    for dim, blocks in pieces:
        steps = jnp.exp(jax.random.uniform(jax.random.fold_in(own, dim), (blocks,), jnp.float32, smallest / len(pieces), high / len(pieces)))
        loudness = loudness * jnp.repeat(steps, dims[dim] // blocks).reshape([-1 if axis == dim else 1 for axis in range(len(dims))])
    return loudness


def noise(own_key, shape, spread, bound, split=(), held_as=jnp.bfloat16):
    array = spread * jax.random.normal(own_key, shape, jnp.float32)
    if split:
        array = array * steps_of(own_key, shape, split, -0.22, 0.18)
    return jnp.clip(array, -bound, bound).astype(held_as)


def setup_inputs(seed: int = 0) -> dict:
    key_of = jax.random.split(jax.random.key(seed), 6)
    return {
        "coords": noise(key_of[0], (NBLK, 3, BA), 0.5, 3.0, ((0, 32),), jnp.float32),
        "force": draw_force(jax.random.fold_in(key_of[5], 71), 0),
        "restraint": jnp.clip(jnp.exp(math.log(4.0) - 2.7725887 * jax.random.uniform(key_of[2], (NBLK, BA), jnp.float32) ** steps_of(key_of[2], (NBLK, BA), ((0, 32),), -0.2, 0.2)), 0.25, 4.0),
        "neighbors": draw_neighbors(jax.random.fold_in(key_of[5], 71), 0),
        "mask": draw_mask(jax.random.fold_in(key_of[5], 71), 0),
    }


def block_product(own_coords, own_values, own_spring, far_coords, far_values, live_flags):
    offset = far_coords[:, :, None, :] - own_coords[None, :, :, None]
    squared = jnp.sum(offset * offset, axis=1)
    soften = 1.0 + squared
    weight = live_flags[:, None, None] / (own_coords.shape[-1] * soften * soften)
    motion = jnp.sum(offset * (own_values[None, :, :, None] - far_values[:, :, None, :]), axis=1)
    strength = weight * motion
    pulled = jnp.sum(strength[:, None, :, :] * offset, axis=(0, 3))
    return own_spring[None, :] * own_values + pulled


def apply_operator(vector, coords, restraint, neighbors, live_mask):
    def one_block(packed):
        own_coords, own_values, own_spring, near_rows, live_flags = packed
        near_rows = near_rows.astype(jnp.int32)
        return block_product(own_coords, own_values, own_spring, coords[near_rows], vector[near_rows], live_flags)

    return lax.map(one_block, (coords, vector, restraint, neighbors, live_mask))


def reference(coords, force, restraint, neighbors, mask):
    live_mask = mask.astype(jnp.float32)
    solution = jnp.zeros_like(force)
    residual = force
    direction = force
    norm_now = jnp.sum(residual * residual)
    for iteration in range(ITERS):
        image = apply_operator(direction, coords, restraint, neighbors, live_mask)
        step_size = norm_now / jnp.sum(direction * image)
        solution = solution + step_size * direction
        residual = residual - step_size * image
        if iteration + 1 < ITERS:
            norm_next = jnp.sum(residual * residual)
            direction = residual + (norm_next / norm_now) * direction
            norm_now = norm_next
    return solution, residual
```

```python
import functools
import jax
import jax.numpy as jnp
from jax import lax
from jax.experimental import pallas as pl
from jax.experimental.pallas import tpu as pltpu
from jax.sharding import PartitionSpec as P

F32 = jnp.float32
BF16 = jnp.bfloat16
DEAD = 2.0 ** 100
FEATS = 32


def vmem():
    return pl.BlockSpec(memory_space=pltpu.VMEM)


def split3(x):
    h = x.astype(BF16).astype(F32)
    rest = x - h
    m = rest.astype(BF16).astype(F32)
    return h, m, (rest - m).astype(BF16).astype(F32)


def rows_iota():
    return lax.broadcasted_iota(jnp.int32, (8, 128), 0)


def sel4(a, b, c, d):
    k = rows_iota() & 3
    return jnp.where(k == 0, a, jnp.where(k == 1, b, jnp.where(k == 2, c, d)))


def spread(row):
    return jnp.broadcast_to(row, (8, 128))


def read3(ref, c, first=0):
    return [spread(ref[c, first + a : first + a + 1, :]) for a in range(3)]


def centred(xs, centre):
    return [x - centre[a] for a, x in enumerate(xs)]


def products(xs, last4):
    ri = rows_iota()
    one_x0 = jnp.where(ri < 4, 1.0, xs[0])
    x1_x2 = jnp.where(ri < 4, xs[1], xs[2])
    return one_x0 * last4, x1_x2 * last4


def dot3(a, b):
    return a[0] * b[0] + a[1] * b[1] + a[2] * b[2]


def put_features(ref, c, xs, vs, with_self):
    groups = list(products(xs, sel4(vs[0], vs[1], vs[2], dot3(xs, vs))))
    if with_self:
        groups += list(products(xs, sel4(xs[0], xs[1], xs[2], 1.0)))
    x = jnp.concatenate(groups, axis=0)
    h, m, low = split3(x)
    ref[c // 2, :, 128 * (c % 2) : 128 * (c % 2) + 128] = jnp.concatenate([h, m, low], axis=0).astype(BF16)


def put_far_side(ref, c, xs):
    ri = rows_iota()
    h, m, low = split3(sel4(xs[0], xs[1], xs[2], dot3(xs, xs)))
    mark = (lax.broadcasted_iota(jnp.int32, (FEATS, 128), 0) == c).astype(F32)
    x = jnp.concatenate([h, m, jnp.where(ri < 4, low, 1.0), h, mark], axis=0)
    ref[c] = x.T.astype(BF16)


def put_own_side(ref, b, xs, dead):
    ri = rows_iota()
    h, m, low = split3(sel4(xs[0], xs[1], xs[2], 0.0))
    nh, nm, nl = split3(1.0 + dot3(xs, xs))
    first = jnp.where(ri == 3, 1.0, jnp.where(ri < 4, -2.0 * h, -2.0 * m))
    first = jnp.where(ri == 7, 0.0, first)
    third = jnp.where(ri < 3, -2.0 * h, jnp.where(ri == 3, 1.0, sel4(nh, nm, nl, 0.0)))
    fourth = jnp.where(ri < 3, -2.0 * low, 0.0)
    x = jnp.concatenate([first, first, third, fourth, dead], axis=0)
    ref[b // 2, :, 128 * (b % 2) : 128 * (b % 2) + 128] = x.astype(BF16)


def dead_rows(near_ref, mask_ref, b, base, slots):
    h = lax.broadcasted_iota(jnp.int32, (FEATS, slots), 0)
    near = jnp.broadcast_to(near_ref[b : b + 1, :], (FEATS, slots))
    live = jnp.broadcast_to(mask_ref[b : b + 1, :], (FEATS, slots)) > 0
    hit = jnp.where(live & (near == base(h)), 1.0, 0.0)
    found = jnp.max(hit, axis=1, keepdims=True)
    return jnp.broadcast_to((1.0 - found) * DEAD, (FEATS, 128))


def pair_weights(far, own):
    s = jnp.dot(far, own, preferred_element_type=F32)
    r = 1.0 / s
    w = r * r
    hi = w.astype(BF16)
    return hi, (w - hi.astype(F32)).astype(BF16)


def fold(acc, n):
    both = acc[:, :128] + acc[:, 128:]
    return (both[:n] + both[n : 2 * n] + both[2 * n :]) * (1.0 / 128)


def first_product(weights_ref, far_side, own_side, feats, put, pairs, window):
    def step(p, carry):
        own = own_side[p]
        start = p if window else 0
        accs = [jnp.zeros((3 * FEATS, 256), F32) for _ in range(2)]
        for t in range(pairs):
            parts = [[], []]
            for cc in range(2):
                hi, lo = pair_weights(far_side[2 * (start + t) + cc], own)
                for q in range(2):
                    cut = slice(128 * q, 128 * q + 128)
                    parts[q].append(jnp.concatenate([hi[:, cut], lo[:, cut]], axis=1))
            f = feats[start + t]
            for q in range(2):
                tile = jnp.concatenate(parts[q], axis=0)
                weights_ref[2 * p + q, t] = tile
                accs[q] = accs[q] + jnp.dot(f, tile, preferred_element_type=F32)
        for q in range(2):
            put(2 * p + q, fold(accs[q], FEATS))
        return carry

    lax.fori_loop(0, pairs, step, 0)


def second_product(weights_ref, feats, put, pairs, window):
    def step(p, carry):
        start = p if window else 0
        for q in range(2):
            acc = jnp.zeros((3 * FEATS // 2, 256), F32)
            for t in range(pairs):
                acc = acc + jnp.dot(feats[start + t], weights_ref[2 * p + q, t], preferred_element_type=F32)
            put(2 * p + q, fold(acc, FEATS // 2))
        return carry

    lax.fori_loop(0, pairs, step, 0)


def apply_local(field, feld_self, xs, vs, stiff, residual_rows):
    q = dot3(xs, vs)
    vpat = sel4(vs[0], vs[1], vs[2], -q)
    xpat = sel4(xs[0], xs[1], xs[2], -1.0)
    g01 = feld_self[0:8] * vpat + field[0:8] * xpat
    g23 = feld_self[8:16] * vpat + field[8:16] * xpat
    z = [jnp.sum(g, axis=0, keepdims=True) for g in (g01[0:4], g01[4:8], g23[0:4], g23[4:8])]
    for a in range(3):
        residual_rows(a, stiff * vs[a][0:1] + z[a + 1] - xs[a][0:1] * z[0])


def local_first(coords, force, near, mask, weights, field, centre_out, far_side, own_side, feats):
    blocks, _, atoms = coords.shape
    slots = near.shape[1]
    first_block = lax.axis_index("space") * blocks
    total = coords[0]
    for b in range(1, blocks):
        total = total + coords[b]
    mean = jnp.sum(total, axis=1, keepdims=True) * (1.0 / (blocks * atoms))
    centre = [jnp.broadcast_to(mean[a : a + 1], (8, 128)) for a in range(3)]
    for a in range(3):
        centre_out[8 * a : 8 * a + 8] = centre[a]
    for b in range(blocks):
        xs = centred(read3(coords, b), centre)
        put_far_side(far_side, b, xs)
        put_features(feats, b, xs, read3(force, b), True)
        put_own_side(own_side, b, xs, dead_rows(near, mask, b, lambda h: h + first_block, slots))

    def put(b, value):
        field[b] = value

    first_product(weights, far_side, own_side, feats, put, blocks // 2, False)


def get_centre(ref):
    return [ref[8 * a : 8 * a + 8] for a in range(3)]


def halo(left, right, c, blocks):
    return (left, c + 1) if c < blocks - 1 else (right, c - (blocks - 1))


def halo_first(left, right, coords, force, stiff, near, mask, centre_in, field_in, weights, selfs, image, far_side, own_side, feats):
    blocks = coords.shape[0]
    slots = near.shape[1]
    first_block = lax.axis_index("space") * blocks
    centre = get_centre(centre_in)
    base = lambda h: first_block + h + jnp.where(h < blocks - 1, 1 - blocks, 1)
    for c in range(2 * (blocks - 1)):
        ref, k = halo(left, right, c, blocks)
        xs = centred(read3(ref, k), centre)
        put_far_side(far_side, c, xs)
        put_features(feats, c, xs, read3(ref, k, 3), True)
    for b in range(blocks):
        xs = centred(read3(coords, b), centre)
        put_own_side(own_side, b, xs, dead_rows(near, mask, b, base, slots))

    def put(b, value):
        value = value + field_in[b]
        half = FEATS // 2
        selfs[b] = value[half:]
        xs = centred(read3(coords, b), centre)

        def rows(a, row):
            image[b, a : a + 1, :] = row

        apply_local(value[:half], value[half:], xs, read3(force, b), stiff[pl.ds(b, 1), :], rows)

    first_product(weights, far_side, own_side, feats, put, blocks // 2, True)


def local_second(coords, vector, centre_in, weights, field, feats):
    blocks = coords.shape[0]
    centre = get_centre(centre_in)
    for b in range(blocks):
        put_features(feats, b, centred(read3(coords, b), centre), read3(vector, b), False)

    def put(b, value):
        field[b] = value

    second_product(weights, feats, put, blocks // 2, False)


def total(x):
    return jnp.sum(jnp.sum(x, axis=0, keepdims=True), axis=1, keepdims=True)


def halo_second(vleft, vright, left, right, coords, vector, force, stiff, centre_in, selfs, field_in, weights, image, sums, feats):
    blocks = coords.shape[0]
    centre = get_centre(centre_in)
    for c in range(2 * (blocks - 1)):
        ref, k = halo(left, right, c, blocks)
        vref, _ = halo(vleft, vright, c, blocks)
        put_features(feats, c, centred(read3(ref, k), centre), read3(vref, k), False)

    def put(b, value):
        value = value + field_in[b]
        xs = centred(read3(coords, b), centre)

        def rows(a, row):
            image[b, a : a + 1, :] = row

        apply_local(value, selfs[b], xs, read3(vector, b), stiff[pl.ds(b, 1), :], rows)

    second_product(weights, feats, put, blocks // 2, True)
    s00 = s01 = jnp.zeros(force.shape[1:], F32)
    for b in range(blocks):
        f, v = force[b], vector[b]
        s00 = s00 + f * f
        s01 = s01 + f * v
    s00, s01 = total(s00), total(s01)
    shift = s01 / jnp.maximum(s00, 1e-30)
    parts = [jnp.zeros(force.shape[1:], F32) for _ in range(4)]
    for b in range(blocks):
        f, v, w = force[b], vector[b], image[b]
        u = v - shift * f
        w = w - shift * v
        for k, term in enumerate((f * u, u * u, f * w + u * v, u * w)):
            parts[k] = parts[k] + term
    values = [s00, s01, shift] + [total(x) for x in parts]
    lane = lax.broadcasted_iota(jnp.int32, sums.shape, 1)
    row = jnp.zeros(sums.shape, F32)
    for k, value in enumerate(values):
        row = jnp.where(lane == k, value, row)
    sums[...] = row


def finish(sums, force, image, image2, solution_out, residual_out):
    table = sums[...]
    s00, s01, shift, s0u, suu, cross, suw = [table[:, k : k + 1] for k in range(7)]
    add = lambda x: jnp.sum(x, axis=0, keepdims=True)
    norm = add(s00)
    alpha = norm / add(s01)
    e = 1.0 - alpha * shift
    norm1 = add(e * e * s00 - 2.0 * alpha * e * s0u + alpha * alpha * suu)
    curve = add(e * e * s01 - alpha * e * cross + alpha * alpha * suw)
    beta = norm1 / norm
    step = norm1 / (curve - beta * norm1 / alpha)
    for b in range(force.shape[0]):
        f, v, w = force[b], image[b], image2[b]
        r = f - alpha * v
        solution_out[b] = alpha * f + step * (r + beta * f)
        residual_out[b] = r - step * (v - alpha * w + beta * v)


def params():
    return pltpu.CompilerParams(vmem_limit_bytes=8 * 2 ** 20)


def call(kernel, outs, args, scratch=()):
    return pl.pallas_call(
        kernel,
        out_shape=[jax.ShapeDtypeStruct(s, d) for s, d in outs],
        in_specs=[vmem()] * len(args),
        out_specs=[vmem()] * len(outs),
        scratch_shapes=[pltpu.VMEM(s, d) for s, d in scratch],
        compiler_params=params(),
    )(*args)


def per_device(coords, force, restraint, neighbors, mask):
    blocks, _, atoms = coords.shape
    devices = lax.axis_size("space")
    up = [(i, i + 1) for i in range(devices - 1)]
    down = [(i + 1, i) for i in range(devices - 1)]
    both = jnp.concatenate([coords, force], axis=1)
    left = lax.ppermute(both, "space", up)
    right = lax.ppermute(both, "space", down)
    wshape = ((blocks, blocks // 2, 2 * atoms, 2 * atoms), BF16)
    own_scratch = ((blocks // 2, 2 * FEATS, 2 * atoms), BF16)
    far = blocks * 2 - 2
    vec = (coords.shape, F32)

    w1, field, centre = call(
        local_first,
        [wshape, ((blocks, FEATS, atoms), F32), ((24, 128), F32)],
        (coords, force, neighbors, mask),
        [((blocks, atoms, 2 * FEATS), BF16), own_scratch, ((blocks // 2, 3 * FEATS, 2 * atoms), BF16)],
    )
    w2, selfs, image = call(
        halo_first,
        [wshape, ((blocks, FEATS // 2, atoms), F32), vec],
        (left, right, coords, force, restraint, neighbors, mask, centre, field),
        [((far, atoms, 2 * FEATS), BF16), own_scratch, ((far // 2, 3 * FEATS, 2 * atoms), BF16)],
    )
    vleft = lax.ppermute(image, "space", up)
    vright = lax.ppermute(image, "space", down)
    (field2,) = call(
        local_second,
        [((blocks, FEATS // 2, atoms), F32)],
        (coords, image, centre, w1),
        [((blocks // 2, 3 * FEATS // 2, 2 * atoms), BF16)],
    )
    image2, sums = call(
        halo_second,
        [vec, ((devices, 128), F32)],
        (vleft, vright, left, right, coords, image, force, restraint, centre, selfs, field2, w2),
        [((far // 2, 3 * FEATS // 2, 2 * atoms), BF16)],
    )
    table = lax.all_to_all(sums, "space", 0, 0, tiled=True)
    solved, residual = call(finish, [vec, vec], (table, force, image, image2))
    return solved, residual


def solution(mesh):
    in_specs = (
        P("space", None, None),
        P("space", None, None),
        P("space", None),
        P("space", None),
        P("space", None),
    )
    out_specs = (P("space", None, None), P("space", None, None))
    return jax.shard_map(per_device, mesh=mesh, in_specs=in_specs, out_specs=out_specs, check_vma=False)
```

```python
import functools
import jax
import jax.numpy as jnp
from jax import lax
from jax.experimental import pallas as pl
from jax.experimental.pallas import tpu as pltpu
from jax.sharding import PartitionSpec as P

F32 = jnp.float32
BF16 = jnp.bfloat16
DEAD = 2.0 ** 100
FEATS = 32


def vmem():
    return pl.BlockSpec(memory_space=pltpu.VMEM)


def split3(x):
    h = x.astype(BF16).astype(F32)
    rest = x - h
    m = rest.astype(BF16).astype(F32)
    return h, m, (rest - m).astype(BF16).astype(F32)


def rows_iota():
    return lax.broadcasted_iota(jnp.int32, (8, 128), 0)


def sel4(a, b, c, d):
    k = rows_iota() & 3
    return jnp.where(k == 0, a, jnp.where(k == 1, b, jnp.where(k == 2, c, d)))


def spread(row):
    return jnp.broadcast_to(row, (8, 128))


def read3(ref, c, first=0):
    return [spread(ref[c, first + a : first + a + 1, :]) for a in range(3)]


def centred(xs, centre):
    return [x - centre[a] for a, x in enumerate(xs)]


def products(xs, last4):
    ri = rows_iota()
    one_x0 = jnp.where(ri < 4, 1.0, xs[0])
    x1_x2 = jnp.where(ri < 4, xs[1], xs[2])
    return one_x0 * last4, x1_x2 * last4


def dot3(a, b):
    return a[0] * b[0] + a[1] * b[1] + a[2] * b[2]


def put_features(ref, c, xs, vs, with_self):
    groups = list(products(xs, sel4(vs[0], vs[1], vs[2], dot3(xs, vs))))
    if with_self:
        groups += list(products(xs, sel4(xs[0], xs[1], xs[2], 1.0)))
    x = jnp.concatenate(groups, axis=0)
    h, m, low = split3(x)
    ref[c] = jnp.concatenate([h, m, low], axis=0).astype(BF16)


def put_far_side(ref, c, xs):
    ri = rows_iota()
    h, m, low = split3(sel4(xs[0], xs[1], xs[2], dot3(xs, xs)))
    mark = (lax.broadcasted_iota(jnp.int32, (FEATS, 128), 0) == c).astype(F32)
    rest = jnp.zeros((128 - 2 * FEATS, 128), F32)
    x = jnp.concatenate([h, m, jnp.where(ri < 4, low, 1.0), h, mark, rest], axis=0)
    ref[c] = x.astype(BF16).T


def put_own_side(ref, b, xs, dead):
    ri = rows_iota()
    h, m, low = split3(sel4(xs[0], xs[1], xs[2], 0.0))
    nh, nm, nl = split3(1.0 + dot3(xs, xs))
    first = jnp.where(ri == 3, 1.0, jnp.where(ri < 4, -2.0 * h, -2.0 * m))
    first = jnp.where(ri == 7, 0.0, first)
    third = jnp.where(ri < 3, -2.0 * h, jnp.where(ri == 3, 1.0, sel4(nh, nm, nl, 0.0)))
    fourth = jnp.where(ri < 3, -2.0 * low, 0.0)
    x = jnp.concatenate([first, first, third, fourth, dead], axis=0)
    ref[b] = x.astype(BF16)


def dead_rows(near_ref, mask_ref, b, base, slots):
    h = lax.broadcasted_iota(jnp.int32, (FEATS, slots), 0)
    near = jnp.broadcast_to(near_ref[b : b + 1, :], (FEATS, slots))
    live = jnp.broadcast_to(mask_ref[b : b + 1, :], (FEATS, slots)) > 0
    hit = jnp.where(live & (near == base(h)), 1.0, 0.0)
    found = jnp.max(hit, axis=1, keepdims=True)
    return jnp.broadcast_to((1.0 - found) * DEAD, (FEATS, 128))


def fold(acc, n):
    both = acc[:, :128] + acc[:, 128:]
    return (both[:n] + both[n : 2 * n] + both[2 * n :]) * (1.0 / 128)


def beside(a, b):
    return jnp.concatenate([a, b], axis=1)


def first_product(weights_ref, far_side, own_side, feats, put, pairs, window):
    depth = 4

    def body(*accs):
        soft, outs = accs[:depth], accs[depth:]

        def push_own(p):
            own = beside(own_side[2 * p], own_side[2 * p + 1])
            own = jnp.concatenate([own, jnp.zeros((256 - own.shape[0], 256), BF16)], axis=0)
            pltpu.matmul_push_rhs(own, staging_register=p % 2, mxu_index=0)

        push_own(0)
        for p in range(pairs):
            start = p if window else 0
            for t in range(pairs):
                parts = [[], []]
                for cc in range(2):
                    first = t + cc == 0
                    far = far_side[2 * (start + t) + cc]
                    acc = soft[(2 * t + cc) % depth]
                    pltpu.matmul_acc_lhs(acc, beside(far, far), load_staged_rhs=p % 2 if first else None)
                    if first and p + 1 < pairs:
                        push_own(p + 1)
                    r = 1.0 / pltpu.matmul_pop(acc)
                    w = r * r
                    hi = w.astype(BF16)
                    lo = (w - hi.astype(F32)).astype(BF16)
                    rows = slice(128 * cc, 128 * cc + 128)
                    for q in range(2):
                        cut = slice(128 * q, 128 * q + 128)
                        weights_ref[2 * p + q, t, 0, rows] = hi[:, cut]
                        weights_ref[2 * p + q, t, 1, rows] = lo[:, cut]
                        parts[q].append(beside(hi[:, cut], lo[:, cut]))
                f = beside(feats[2 * (start + t)], feats[2 * (start + t) + 1])
                for q in range(2):
                    pltpu.matmul_push_rhs(jnp.concatenate(parts[q], axis=0), staging_register=q, mxu_index=1)
                    pltpu.matmul_acc_lhs(outs[2 * (p % 2) + q], f, load_staged_rhs=q)
            for q in range(2):
                put(2 * p + q, fold(pltpu.matmul_pop(outs[2 * (p % 2) + q]), FEATS))

    soft = [pltpu.ACC(0)((128, 256), F32) for _ in range(depth)]
    outs = [pltpu.ACC(1)((3 * FEATS, 256), F32) for _ in range(4)]
    pl.run_scoped(body, *soft, *outs)


def second_product(weights_ref, feats, put, pairs, window):
    rows = 3 * FEATS // 2

    def body(*accs):
        for p in range(pairs):
            start = p if window else 0
            for t in range(pairs):
                f = beside(feats[2 * (start + t)], feats[2 * (start + t) + 1])
                for q in range(2):
                    tile = beside(weights_ref[2 * p + q, t, 0], weights_ref[2 * p + q, t, 1])
                    pltpu.matmul_push_rhs(tile, staging_register=t % 2, mxu_index=q)
                    pltpu.matmul_acc_lhs(accs[2 * q + p % 2], f, load_staged_rhs=t % 2)
            for q in range(2):
                put(2 * p + q, fold(pltpu.matmul_pop(accs[2 * q + p % 2]), FEATS // 2))

    pl.run_scoped(body, *[pltpu.ACC(q)((rows, 256), F32) for q in (0, 0, 1, 1)])


def apply_local(field, feld_self, xs, vs, stiff, residual_rows):
    q = dot3(xs, vs)
    vpat = sel4(vs[0], vs[1], vs[2], -q)
    xpat = sel4(xs[0], xs[1], xs[2], -1.0)
    g01 = feld_self[0:8] * vpat + field[0:8] * xpat
    g23 = feld_self[8:16] * vpat + field[8:16] * xpat
    z = [jnp.sum(g, axis=0, keepdims=True) for g in (g01[0:4], g01[4:8], g23[0:4], g23[4:8])]
    for a in range(3):
        residual_rows(a, stiff * vs[a][0:1] + z[a + 1] - xs[a][0:1] * z[0])


def local_first(coords, force, near, mask, weights, field, centre_out, far_side, own_side, feats):
    blocks, _, atoms = coords.shape
    slots = near.shape[1]
    first_block = lax.axis_index("space") * blocks
    total = coords[0]
    for b in range(1, blocks):
        total = total + coords[b]
    mean = jnp.sum(total, axis=1, keepdims=True) * (1.0 / (blocks * atoms))
    centre = [jnp.broadcast_to(mean[a : a + 1], (8, 128)) for a in range(3)]
    for a in range(3):
        centre_out[8 * a : 8 * a + 8] = centre[a]
    for b in range(blocks):
        xs = centred(read3(coords, b), centre)
        put_far_side(far_side, b, xs)
        put_features(feats, b, xs, read3(force, b), True)
        put_own_side(own_side, b, xs, dead_rows(near, mask, b, lambda h: h + first_block, slots))

    def put(b, value):
        field[b] = value

    first_product(weights, far_side, own_side, feats, put, blocks // 2, False)


def get_centre(ref):
    return [ref[8 * a : 8 * a + 8] for a in range(3)]


def halo(left, right, c, blocks):
    return (left, c + 1) if c < blocks - 1 else (right, c - (blocks - 1))


def halo_first(left, right, coords, force, stiff, near, mask, centre_in, field_in, weights, selfs, image, far_side, own_side, feats):
    blocks = coords.shape[0]
    slots = near.shape[1]
    first_block = lax.axis_index("space") * blocks
    centre = get_centre(centre_in)
    base = lambda h: first_block + h + jnp.where(h < blocks - 1, 1 - blocks, 1)
    for c in range(2 * (blocks - 1)):
        ref, k = halo(left, right, c, blocks)
        xs = centred(read3(ref, k), centre)
        put_far_side(far_side, c, xs)
        put_features(feats, c, xs, read3(ref, k, 3), True)
    for b in range(blocks):
        xs = centred(read3(coords, b), centre)
        put_own_side(own_side, b, xs, dead_rows(near, mask, b, base, slots))

    def put(b, value):
        value = value + field_in[b]
        half = FEATS // 2
        selfs[b] = value[half:]
        xs = centred(read3(coords, b), centre)

        def rows(a, row):
            image[b, a : a + 1, :] = row

        apply_local(value[:half], value[half:], xs, read3(force, b), stiff[pl.ds(b, 1), :], rows)

    first_product(weights, far_side, own_side, feats, put, blocks // 2, True)


def local_second(coords, vector, centre_in, weights, field, feats):
    blocks = coords.shape[0]
    centre = get_centre(centre_in)
    for b in range(blocks):
        put_features(feats, b, centred(read3(coords, b), centre), read3(vector, b), False)

    def put(b, value):
        field[b] = value

    second_product(weights, feats, put, blocks // 2, False)


def total(x):
    return jnp.sum(jnp.sum(x, axis=0, keepdims=True), axis=1, keepdims=True)


def halo_second(vleft, vright, left, right, coords, vector, force, stiff, centre_in, selfs, field_in, weights, image, sums, feats):
    blocks = coords.shape[0]
    centre = get_centre(centre_in)
    for c in range(2 * (blocks - 1)):
        ref, k = halo(left, right, c, blocks)
        vref, _ = halo(vleft, vright, c, blocks)
        put_features(feats, c, centred(read3(ref, k), centre), read3(vref, k), False)

    def put(b, value):
        value = value + field_in[b]
        xs = centred(read3(coords, b), centre)

        def rows(a, row):
            image[b, a : a + 1, :] = row

        apply_local(value, selfs[b], xs, read3(vector, b), stiff[pl.ds(b, 1), :], rows)

    second_product(weights, feats, put, blocks // 2, True)
    s00 = s01 = jnp.zeros(force.shape[1:], F32)
    for b in range(blocks):
        f, v = force[b], vector[b]
        s00 = s00 + f * f
        s01 = s01 + f * v
    s00, s01 = total(s00), total(s01)
    shift = s01 / jnp.maximum(s00, 1e-30)
    parts = [jnp.zeros(force.shape[1:], F32) for _ in range(4)]
    for b in range(blocks):
        f, v, w = force[b], vector[b], image[b]
        u = v - shift * f
        w = w - shift * v
        for k, term in enumerate((f * u, u * u, f * w + u * v, u * w)):
            parts[k] = parts[k] + term
    values = [s00, s01, shift] + [total(x) for x in parts]
    lane = lax.broadcasted_iota(jnp.int32, sums.shape, 1)
    row = jnp.zeros(sums.shape, F32)
    for k, value in enumerate(values):
        row = jnp.where(lane == k, value, row)
    sums[...] = row


def finish(sums, force, image, image2, solution_out, residual_out):
    table = sums[...]
    s00, s01, shift, s0u, suu, cross, suw = [table[:, k : k + 1] for k in range(7)]
    add = lambda x: jnp.sum(x, axis=0, keepdims=True)
    norm = add(s00)
    alpha = norm / add(s01)
    e = 1.0 - alpha * shift
    norm1 = add(e * e * s00 - 2.0 * alpha * e * s0u + alpha * alpha * suu)
    curve = add(e * e * s01 - alpha * e * cross + alpha * alpha * suw)
    beta = norm1 / norm
    step = norm1 / (curve - beta * norm1 / alpha)
    for b in range(force.shape[0]):
        f, v, w = force[b], image[b], image2[b]
        r = f - alpha * v
        solution_out[b] = alpha * f + step * (r + beta * f)
        residual_out[b] = r - step * (v - alpha * w + beta * v)


def params():
    return pltpu.CompilerParams(vmem_limit_bytes=8 * 2 ** 20)


def call(kernel, outs, args, scratch=()):
    return pl.pallas_call(
        kernel,
        out_shape=[jax.ShapeDtypeStruct(s, d) for s, d in outs],
        in_specs=[vmem()] * len(args),
        out_specs=[vmem()] * len(outs),
        scratch_shapes=[pltpu.VMEM(s, d) for s, d in scratch],
        compiler_params=params(),
    )(*args)


def per_device(coords, force, restraint, neighbors, mask):
    blocks, _, atoms = coords.shape
    devices = lax.axis_size("space")
    up = [(i, i + 1) for i in range(devices - 1)]
    down = [(i + 1, i) for i in range(devices - 1)]
    both = jnp.concatenate([coords, force], axis=1)
    left = lax.ppermute(both, "space", up)
    right = lax.ppermute(both, "space", down)
    wshape = ((blocks, blocks // 2, 2, 2 * atoms, atoms), BF16)
    own_scratch = ((blocks, 2 * FEATS, atoms), BF16)
    far = blocks * 2 - 2
    vec = (coords.shape, F32)

    w1, field, centre = call(
        local_first,
        [wshape, ((blocks, FEATS, atoms), F32), ((24, 128), F32)],
        (coords, force, neighbors, mask),
        [((blocks, atoms, atoms), BF16), own_scratch, ((blocks, 3 * FEATS, atoms), BF16)],
    )
    w2, selfs, image = call(
        halo_first,
        [wshape, ((blocks, FEATS // 2, atoms), F32), vec],
        (left, right, coords, force, restraint, neighbors, mask, centre, field),
        [((far, atoms, atoms), BF16), own_scratch, ((far, 3 * FEATS, atoms), BF16)],
    )
    vleft = lax.ppermute(image, "space", up)
    vright = lax.ppermute(image, "space", down)
    (field2,) = call(
        local_second,
        [((blocks, FEATS // 2, atoms), F32)],
        (coords, image, centre, w1),
        [((blocks, 3 * FEATS // 2, atoms), BF16)],
    )
    image2, sums = call(
        halo_second,
        [vec, ((devices, 128), F32)],
        (vleft, vright, left, right, coords, image, force, restraint, centre, selfs, field2, w2),
        [((far, 3 * FEATS // 2, atoms), BF16)],
    )
    table = lax.all_to_all(sums, "space", 0, 0, tiled=True)
    solved, residual = call(finish, [vec, vec], (table, force, image, image2))
    return solved, residual


def solution(mesh):
    in_specs = (
        P("space", None, None),
        P("space", None, None),
        P("space", None),
        P("space", None),
        P("space", None),
    )
    out_specs = (P("space", None, None), P("space", None, None))
    return jax.shard_map(per_device, mesh=mesh, in_specs=in_specs, out_specs=out_specs, check_vma=False)
```

```python
import functools
import jax
import jax.numpy as jnp
from jax import lax
from jax.experimental import pallas as pl
from jax.experimental.pallas import tpu as pltpu
from jax.sharding import PartitionSpec as P

F32 = jnp.float32
BF16 = jnp.bfloat16
DEAD = 2.0 ** 100
FEATS = 32


def vmem():
    return pl.BlockSpec(memory_space=pltpu.VMEM)


def split3(x):
    h = x.astype(BF16).astype(F32)
    rest = x - h
    m = rest.astype(BF16).astype(F32)
    return h, m, (rest - m).astype(BF16).astype(F32)


def rows_iota():
    return lax.broadcasted_iota(jnp.int32, (8, 128), 0)


def sel4(a, b, c, d):
    k = rows_iota() & 3
    return jnp.where(k == 0, a, jnp.where(k == 1, b, jnp.where(k == 2, c, d)))


def spread(row):
    return jnp.broadcast_to(row, (8, 128))


def read3(ref, c, first=0):
    return [spread(ref[first + a, pl.ds(c, 1), :]) for a in range(3)]


def centred(xs, centre):
    return [x - centre[a] for a, x in enumerate(xs)]


def products(xs, last4):
    ri = rows_iota()
    one_x0 = jnp.where(ri < 4, 1.0, xs[0])
    x1_x2 = jnp.where(ri < 4, xs[1], xs[2])
    return one_x0 * last4, x1_x2 * last4


def dot3(a, b):
    return a[0] * b[0] + a[1] * b[1] + a[2] * b[2]


def put_features(ref, c, xs, vs, with_self):
    groups = list(products(xs, sel4(vs[0], vs[1], vs[2], dot3(xs, vs))))
    if with_self:
        groups += list(products(xs, sel4(xs[0], xs[1], xs[2], 1.0)))
    x = jnp.concatenate(groups, axis=0)
    h, m, low = split3(x)
    ref[c] = jnp.concatenate([h, m, low], axis=0).astype(BF16)


def put_far_side(ref, c, xs):
    ri = rows_iota()
    h, m, low = split3(sel4(xs[0], xs[1], xs[2], dot3(xs, xs)))
    mark = (lax.broadcasted_iota(jnp.int32, (FEATS, 128), 0) == c).astype(F32)
    rest = jnp.zeros((128 - 2 * FEATS, 128), F32)
    x = jnp.concatenate([h, m, jnp.where(ri < 4, low, 1.0), h, mark, rest], axis=0)
    ref[c] = x.astype(BF16).T


def put_own_side(ref, b, xs, dead):
    ri = rows_iota()
    h, m, low = split3(sel4(xs[0], xs[1], xs[2], 0.0))
    nh, nm, nl = split3(1.0 + dot3(xs, xs))
    first = jnp.where(ri == 3, 1.0, jnp.where(ri < 4, -2.0 * h, -2.0 * m))
    first = jnp.where(ri == 7, 0.0, first)
    third = jnp.where(ri < 3, -2.0 * h, jnp.where(ri == 3, 1.0, sel4(nh, nm, nl, 0.0)))
    fourth = jnp.where(ri < 3, -2.0 * low, 0.0)
    x = jnp.concatenate([first, first, third, fourth, dead], axis=0)
    ref[b] = x.astype(BF16)


def dead_rows(near_ref, mask_ref, b, base, slots):
    h = lax.broadcasted_iota(jnp.int32, (FEATS, slots), 0)
    near = jnp.broadcast_to(near_ref[b : b + 1, :], (FEATS, slots))
    live = jnp.broadcast_to(mask_ref[b : b + 1, :], (FEATS, slots)) > 0
    hit = jnp.where(live & (near == base(h)), 1.0, 0.0)
    found = jnp.max(hit, axis=1, keepdims=True)
    return jnp.broadcast_to((1.0 - found) * DEAD, (FEATS, 128))


def fold(acc, n):
    both = acc[:, :128] + acc[:, 128:]
    return (both[:n] + both[n : 2 * n] + both[2 * n :]) * (1.0 / 128)


def beside(a, b):
    return jnp.concatenate([a, b], axis=1)


def first_product(weights_ref, far_side, own_side, feats, put, pairs, window):
    depth = 4

    def body(*accs):
        soft, outs = accs[:depth], accs[depth:]

        def push_own(p):
            own = beside(own_side[2 * p], own_side[2 * p + 1])
            own = jnp.concatenate([own, jnp.zeros((256 - own.shape[0], 256), BF16)], axis=0)
            pltpu.matmul_push_rhs(own, staging_register=p % 2, mxu_index=0)

        push_own(0)
        for p in range(pairs):
            start = p if window else 0
            for t in range(pairs):
                parts = [[], []]
                for cc in range(2):
                    first = t + cc == 0
                    far = far_side[2 * (start + t) + cc]
                    acc = soft[(2 * t + cc) % depth]
                    pltpu.matmul_acc_lhs(acc, beside(far, far), load_staged_rhs=p % 2 if first else None)
                    if first and p + 1 < pairs:
                        push_own(p + 1)
                    r = 1.0 / pltpu.matmul_pop(acc)
                    w = r * r
                    hi = w.astype(BF16)
                    lo = (w - hi.astype(F32)).astype(BF16)
                    rows = slice(128 * cc, 128 * cc + 128)
                    for q in range(2):
                        cut = slice(128 * q, 128 * q + 128)
                        weights_ref[2 * p + q, t, 0, rows] = hi[:, cut]
                        weights_ref[2 * p + q, t, 1, rows] = lo[:, cut]
                        parts[q].append(beside(hi[:, cut], lo[:, cut]))
                f = beside(feats[2 * (start + t)], feats[2 * (start + t) + 1])
                for q in range(2):
                    pltpu.matmul_push_rhs(jnp.concatenate(parts[q], axis=0), staging_register=q, mxu_index=1)
                    pltpu.matmul_acc_lhs(outs[2 * (p % 2) + q], f, load_staged_rhs=q)
            for q in range(2):
                put(2 * p + q, fold(pltpu.matmul_pop(outs[2 * (p % 2) + q]), FEATS))

    soft = [pltpu.ACC(0)((128, 256), F32) for _ in range(depth)]
    outs = [pltpu.ACC(1)((3 * FEATS, 256), F32) for _ in range(4)]
    pl.run_scoped(body, *soft, *outs)


def second_product(weights_ref, feats, put, pairs, window):
    rows = 3 * FEATS // 2

    def body(*accs):
        for p in range(pairs):
            start = p if window else 0
            for t in range(pairs):
                f = beside(feats[2 * (start + t)], feats[2 * (start + t) + 1])
                for q in range(2):
                    tile = beside(weights_ref[2 * p + q, t, 0], weights_ref[2 * p + q, t, 1])
                    pltpu.matmul_push_rhs(tile, staging_register=t % 2, mxu_index=q)
                    pltpu.matmul_acc_lhs(accs[2 * q + p % 2], f, load_staged_rhs=t % 2)
            for q in range(2):
                put(2 * p + q, fold(pltpu.matmul_pop(accs[2 * q + p % 2]), FEATS // 2))

    pl.run_scoped(body, *[pltpu.ACC(q)((rows, 256), F32) for q in (0, 0, 1, 1)])


def apply_local(field, feld_self, xs, vs, stiff, residual_rows):
    q = dot3(xs, vs)
    vpat = sel4(vs[0], vs[1], vs[2], -q)
    xpat = sel4(xs[0], xs[1], xs[2], -1.0)
    g01 = feld_self[0:8] * vpat + field[0:8] * xpat
    g23 = feld_self[8:16] * vpat + field[8:16] * xpat
    z = [jnp.sum(g, axis=0, keepdims=True) for g in (g01[0:4], g01[4:8], g23[0:4], g23[4:8])]
    for a in range(3):
        residual_rows(a, stiff * vs[a][0:1] + z[a + 1] - xs[a][0:1] * z[0])


def stage(coords, force, stiff, near, mask, both_out, stiff_out, near_out, mask_out, sems):
    copies = (
        (coords, both_out.at[0:3]),
        (force, both_out.at[3:6]),
        (stiff, stiff_out),
        (near, near_out),
        (mask, mask_out),
    )
    started = [pltpu.make_async_copy(src, dst, sems.at[k]) for k, (src, dst) in enumerate(copies)]
    for copy in started:
        copy.start()
    for copy in started:
        copy.wait()


def local_first(both, near, mask, weights, field, centre_out, far_side, own_side, feats):
    _, blocks, atoms = both.shape
    slots = near.shape[1]
    first_block = lax.axis_index("space") * blocks
    centre = [jnp.broadcast_to(total(both[a]) * (1.0 / (blocks * atoms)), (8, 128)) for a in range(3)]
    for a in range(3):
        centre_out[8 * a : 8 * a + 8] = centre[a]
    for b in range(blocks):
        xs = centred(read3(both, b), centre)
        put_far_side(far_side, b, xs)
        put_features(feats, b, xs, read3(both, b, 3), True)
        put_own_side(own_side, b, xs, dead_rows(near, mask, b, lambda h: h + first_block, slots))

    def put(b, value):
        field[b] = value

    first_product(weights, far_side, own_side, feats, put, blocks // 2, False)


def get_centre(ref):
    return [ref[8 * a : 8 * a + 8] for a in range(3)]


def order_halo(mate, other, ref):
    odd = lax.rem(lax.axis_index("space"), 2) == 1
    a, b = mate[...], other[...]
    ref[0] = jnp.where(odd, a, b)
    ref[1] = jnp.where(odd, b, a)


def halo(ref, c, blocks):
    return (ref.at[0], c + 1) if c < blocks - 1 else (ref.at[1], c - (blocks - 1))


def halo_first(mate, other, both, stiff, near, mask, centre_in, field_in, weights, selfs, image, sides, far_side, own_side, feats):
    _, blocks, _ = both.shape
    slots = near.shape[1]
    first_block = lax.axis_index("space") * blocks
    centre = get_centre(centre_in)
    base = lambda h: first_block + h + jnp.where(h < blocks - 1, 1 - blocks, 1)
    order_halo(mate, other, sides)
    for c in range(2 * (blocks - 1)):
        ref, k = halo(sides, c, blocks)
        xs = centred(read3(ref, k), centre)
        put_far_side(far_side, c, xs)
        put_features(feats, c, xs, read3(ref, k, 3), True)
    for b in range(blocks):
        xs = centred(read3(both, b), centre)
        put_own_side(own_side, b, xs, dead_rows(near, mask, b, base, slots))

    def put(b, value):
        value = value + field_in[b]
        half = FEATS // 2
        selfs[b] = value[half:]
        xs = centred(read3(both, b), centre)

        def rows(a, row):
            image[a, b : b + 1, :] = row

        apply_local(value[:half], value[half:], xs, read3(both, b, 3), stiff[b : b + 1, :], rows)

    first_product(weights, far_side, own_side, feats, put, blocks // 2, True)


def local_second(both, vector, centre_in, weights, field, feats):
    _, blocks, _ = both.shape
    centre = get_centre(centre_in)
    for b in range(blocks):
        put_features(feats, b, centred(read3(both, b), centre), read3(vector, b), False)

    def put(b, value):
        field[b] = value

    second_product(weights, feats, put, blocks // 2, False)


def total(x):
    return jnp.sum(jnp.sum(x, axis=0, keepdims=True), axis=1, keepdims=True)


def halo_second(vmate, vother, mate, other, both, vector, stiff, centre_in, selfs, field_in, weights, image, sums, sides, vsides, feats):
    _, blocks, _ = both.shape
    centre = get_centre(centre_in)
    order_halo(mate, other, sides)
    order_halo(vmate, vother, vsides)
    for c in range(2 * (blocks - 1)):
        ref, k = halo(sides, c, blocks)
        vref, _ = halo(vsides, c, blocks)
        put_features(feats, c, centred(read3(ref, k), centre), read3(vref, k), False)

    def put(b, value):
        value = value + field_in[b]
        xs = centred(read3(both, b), centre)

        def rows(a, row):
            image[a, b : b + 1, :] = row

        apply_local(value, selfs[b], xs, read3(vector, b), stiff[b : b + 1, :], rows)

    second_product(weights, feats, put, blocks // 2, True)
    f, v, w = both[3:6], vector[...], image[...]
    add = lambda x: total(jnp.sum(x, axis=0))
    s00, s01 = add(f * f), add(f * v)
    shift = s01 / jnp.maximum(s00, 1e-30)
    u = v - shift * f
    w = w - shift * v
    values = [s00, s01, shift, add(f * u), add(u * u), add(f * w + u * v), add(u * w)]
    lane = lax.broadcasted_iota(jnp.int32, sums.shape, 1)
    row = jnp.zeros(sums.shape, F32)
    for k, value in enumerate(values):
        row = jnp.where(lane == k, value, row)
    sums[...] = row


def finish(sums, both, image, image2, solution_out, residual_out, solution_buf, residual_buf, sems):
    table = sums[...]
    s00, s01, shift, s0u, suu, cross, suw = [table[:, k : k + 1] for k in range(7)]
    add = lambda x: jnp.sum(x, axis=0, keepdims=True)
    norm = add(s00)
    alpha = norm / add(s01)
    e = 1.0 - alpha * shift
    norm1 = add(e * e * s00 - 2.0 * alpha * e * s0u + alpha * alpha * suu)
    curve = add(e * e * s01 - alpha * e * cross + alpha * alpha * suw)
    beta = norm1 / norm
    step = norm1 / (curve - beta * norm1 / alpha)
    f, v, w = both[3:6], image[...], image2[...]
    r = f - alpha * v
    solution_buf[...] = alpha * f + step * (r + beta * f)
    residual_buf[...] = r - step * (v - alpha * w + beta * v)
    copies = [
        pltpu.make_async_copy(solution_buf, solution_out, sems.at[0]),
        pltpu.make_async_copy(residual_buf, residual_out, sems.at[1]),
    ]
    for copy in copies:
        copy.start()
    for copy in copies:
        copy.wait()


def call(kernel, outs, args, scratch=(), hbm_in=False, hbm_out=False, sems=0):
    hbm = pl.BlockSpec(memory_space=pltpu.HBM)
    return pl.pallas_call(
        kernel,
        out_shape=[jax.ShapeDtypeStruct(s, d) for s, d in outs],
        in_specs=[hbm if hbm_in else vmem()] * len(args),
        out_specs=[hbm if hbm_out else vmem()] * len(outs),
        scratch_shapes=[pltpu.VMEM(s, d) for s, d in scratch] + ([pltpu.SemaphoreType.DMA((sems,))] if sems else []),
        compiler_params=pltpu.CompilerParams(vmem_limit_bytes=8 * 2 ** 20),
    )(*args)


def per_device(coords, force, restraint, neighbors, mask):
    blocks, parts, atoms = coords.shape
    devices = lax.axis_size("space")
    mates = [(i, i ^ 1) for i in range(devices)]
    others = [pair for i in range(1, devices - 1, 2) for pair in ((i, i + 1), (i + 1, i))]
    flip = lambda x: jnp.transpose(x, (1, 0, 2))
    vec = ((parts, blocks, atoms), F32)
    pair = ((2 * parts, blocks, atoms), F32)
    wshape = ((blocks, blocks // 2, 2, 2 * atoms, atoms), BF16)
    own_scratch = ((blocks, 2 * FEATS, atoms), BF16)
    far = blocks * 2 - 2

    both, stiff, near, live = call(
        stage,
        [pair, (restraint.shape, F32), (neighbors.shape, neighbors.dtype), (mask.shape, mask.dtype)],
        [pltpu.with_memory_space_constraint(x, pltpu.HBM) for x in (flip(coords), flip(force), restraint, neighbors, mask)],
        hbm_in=True,
        sems=5,
    )
    other = lax.ppermute(both, "space", others)
    mate = lax.ppermute(both, "space", mates)
    w1, field, centre = call(
        local_first,
        [wshape, ((blocks, FEATS, atoms), F32), ((24, 128), F32)],
        (both, near, live),
        [((blocks, atoms, atoms), BF16), own_scratch, ((blocks, 3 * FEATS, atoms), BF16)],
    )
    w2, selfs, image = call(
        halo_first,
        [wshape, ((blocks, FEATS // 2, atoms), F32), vec],
        (mate, other, both, stiff, near, live, centre, field),
        [((2,) + pair[0], F32), ((far, atoms, atoms), BF16), own_scratch, ((far, 3 * FEATS, atoms), BF16)],
    )
    vother = lax.ppermute(image, "space", others)
    vmate = lax.ppermute(image, "space", mates)
    (field2,) = call(
        local_second,
        [((blocks, FEATS // 2, atoms), F32)],
        (both, image, centre, w1),
        [((blocks, 3 * FEATS // 2, atoms), BF16)],
    )
    image2, sums = call(
        halo_second,
        [vec, ((devices, 128), F32)],
        (vmate, vother, mate, other, both, image, stiff, centre, selfs, field2, w2),
        [((2,) + pair[0], F32), ((2,) + vec[0], F32), ((far, 3 * FEATS // 2, atoms), BF16)],
    )
    table = lax.all_to_all(sums, "space", 0, 0, tiled=True)
    solved, residual = call(finish, [vec, vec], (table, both, image, image2), [vec, vec], hbm_out=True, sems=2)
    return flip(solved), flip(residual)


def solution(mesh):
    in_specs = (
        P("space", None, None),
        P("space", None, None),
        P("space", None),
        P("space", None),
        P("space", None),
    )
    out_specs = (P("space", None, None), P("space", None, None))
    return jax.shard_map(per_device, mesh=mesh, in_specs=in_specs, out_specs=out_specs, check_vma=False)
```

```python
import functools
import jax
import jax.numpy as jnp
from jax import lax
from jax.experimental import pallas as pl
from jax.experimental.pallas import tpu as pltpu
from jax.sharding import PartitionSpec as P

F32 = jnp.float32
BF16 = jnp.bfloat16
DEAD = 2.0 ** 100
FEATS = 32


def vmem():
    return pl.BlockSpec(memory_space=pltpu.VMEM)


def split3(x):
    h = x.astype(BF16).astype(F32)
    rest = x - h
    m = rest.astype(BF16).astype(F32)
    return h, m, (rest - m).astype(BF16).astype(F32)


def rows_iota():
    return lax.broadcasted_iota(jnp.int32, (8, 128), 0)


def sel4(a, b, c, d):
    k = rows_iota() & 3
    return jnp.where(k == 0, a, jnp.where(k == 1, b, jnp.where(k == 2, c, d)))


def spread(row):
    return jnp.broadcast_to(row, (8, 128))


def read3(ref, c, first=0):
    return [spread(ref[first + a, pl.ds(c, 1), :]) for a in range(3)]


def centred(xs, centre):
    return [x - centre[a] for a, x in enumerate(xs)]


def products(xs, last4):
    ri = rows_iota()
    one_x0 = jnp.where(ri < 4, 1.0, xs[0])
    x1_x2 = jnp.where(ri < 4, xs[1], xs[2])
    return one_x0 * last4, x1_x2 * last4


def dot3(a, b):
    return a[0] * b[0] + a[1] * b[1] + a[2] * b[2]


def put_features(ref, c, xs, vs, with_self):
    groups = list(products(xs, sel4(vs[0], vs[1], vs[2], dot3(xs, vs))))
    if with_self:
        groups += list(products(xs, sel4(xs[0], xs[1], xs[2], 1.0)))
    x = jnp.concatenate(groups, axis=0)
    h, m, low = split3(x)
    ref[c] = jnp.concatenate([h, m, low], axis=0).astype(BF16)


def put_far_side(ref, c, xs):
    ri = rows_iota()
    h, m, low = split3(sel4(xs[0], xs[1], xs[2], dot3(xs, xs)))
    mark = (lax.broadcasted_iota(jnp.int32, (FEATS, 128), 0) == c).astype(F32)
    rest = jnp.zeros((128 - 2 * FEATS, 128), F32)
    x = jnp.concatenate([h, m, jnp.where(ri < 4, low, 1.0), h, mark, rest], axis=0)
    ref[c] = x.astype(BF16).T


def put_own_side(ref, b, xs, dead):
    ri = rows_iota()
    h, m, low = split3(sel4(xs[0], xs[1], xs[2], 0.0))
    nh, nm, nl = split3(1.0 + dot3(xs, xs))
    first = jnp.where(ri == 3, 1.0, jnp.where(ri < 4, -2.0 * h, -2.0 * m))
    first = jnp.where(ri == 7, 0.0, first)
    third = jnp.where(ri < 3, -2.0 * h, jnp.where(ri == 3, 1.0, sel4(nh, nm, nl, 0.0)))
    fourth = jnp.where(ri < 3, -2.0 * low, 0.0)
    x = jnp.concatenate([first, first, third, fourth, dead], axis=0)
    ref[b] = x.astype(BF16)


def dead_rows(near_ref, mask_ref, b, base, slots):
    h = lax.broadcasted_iota(jnp.int32, (FEATS, slots), 0)
    near = jnp.broadcast_to(near_ref[b : b + 1, :], (FEATS, slots))
    live = jnp.broadcast_to(mask_ref[b : b + 1, :], (FEATS, slots)) > 0
    hit = jnp.where(live & (near == base(h)), 1.0, 0.0)
    found = jnp.max(hit, axis=1, keepdims=True)
    return jnp.broadcast_to((1.0 - found) * DEAD, (FEATS, 128))


def beside(a, b):
    return jnp.concatenate([a, b], axis=1)


def fold(high, low):
    n = low.shape[0]
    return (high[:n] + high[n : 2 * n] + high[2 * n :] + low) * (1.0 / 128)


def pair_features(feats, k):
    return beside(feats[2 * k], feats[2 * k + 1])


def first_product(weights_ref, far_side, own_side, feats, put, pairs, window):
    depth = 4

    def body(*accs):
        soft, outs = accs[:depth], accs[depth:]

        def push_own(p):
            own = beside(own_side[2 * p], own_side[2 * p + 1])
            own = jnp.concatenate([own, jnp.zeros((256 - own.shape[0], 256), BF16)], axis=0)
            pltpu.matmul_push_rhs(own, staging_register=p % 2, mxu_index=0)

        push_own(0)
        for p in range(pairs):
            start = p if window else 0
            high, low = outs[2 * (p % 2)], outs[2 * (p % 2) + 1]
            for t in range(pairs):
                parts = [[], []]
                for cc in range(2):
                    first = t + cc == 0
                    far = far_side[2 * (start + t) + cc]
                    acc = soft[(2 * t + cc) % depth]
                    pltpu.matmul_acc_lhs(acc, beside(far, far), load_staged_rhs=p % 2 if first else None)
                    if first and p + 1 < pairs:
                        push_own(p + 1)
                    r = 1.0 / pltpu.matmul_pop(acc)
                    w = r * r
                    hi = w.astype(BF16)
                    lo = (w - hi.astype(F32)).astype(BF16)
                    rows = slice(8 * cc, 8 * cc + 8)
                    for k, part in enumerate((hi, lo)):
                        parts[k].append(part)
                        for q in range(2):
                            cut = slice(128 * q, 128 * q + 128)
                            weights_ref[p, t, rows, 2 * k + q] = part[:, cut].reshape(8, 16, 128)
                f = pair_features(feats, start + t)
                for k, (acc, rows) in enumerate(((high, 3 * FEATS), (low, FEATS))):
                    pltpu.matmul_push_rhs(jnp.concatenate(parts[k], axis=0), staging_register=k, mxu_index=1)
                    pltpu.matmul_acc_lhs(acc, f[:rows], load_staged_rhs=k)
            value = fold(pltpu.matmul_pop(high), pltpu.matmul_pop(low))
            for q in range(2):
                put(2 * p + q, value[:, 128 * q : 128 * q + 128])

    soft = [pltpu.ACC(0)((128, 256), F32) for _ in range(depth)]
    outs = [pltpu.ACC(1)((n, 256), F32) for n in (3 * FEATS, FEATS) * 2]
    pl.run_scoped(body, *soft, *outs)


def second_product(weights_ref, feats, put, pairs, window):
    half = FEATS // 2

    def body(*accs):
        for first in range(0, pairs, 2):
            turn = accs[4 * (first // 2 % 2) : 4 * (first // 2 % 2) + 4]
            for t in range(pairs):
                for q in range(2):
                    p = first + q
                    f = pair_features(feats, (p if window else 0) + t)
                    for k, rows in enumerate((3 * half, half)):
                        tile = beside(*[weights_ref[p, t, :, 2 * k + i].reshape(256, 128) for i in range(2)])
                        pltpu.matmul_push_rhs(tile, staging_register=k, mxu_index=q)
                        pltpu.matmul_acc_lhs(turn[2 * q + k], f[:rows], load_staged_rhs=k)
            for q in range(2):
                value = fold(pltpu.matmul_pop(turn[2 * q]), pltpu.matmul_pop(turn[2 * q + 1]))
                for i in range(2):
                    put(2 * (first + q) + i, value[:, 128 * i : 128 * i + 128])

    accs = [pltpu.ACC(q)((n, 256), F32) for _ in range(2) for q in range(2) for n in (3 * half, half)]
    pl.run_scoped(body, *accs)


def apply_local(field, feld_self, xs, vs, stiff, residual_rows):
    q = dot3(xs, vs)
    vpat = sel4(vs[0], vs[1], vs[2], -q)
    xpat = sel4(xs[0], xs[1], xs[2], -1.0)
    g01 = feld_self[0:8] * vpat + field[0:8] * xpat
    g23 = feld_self[8:16] * vpat + field[8:16] * xpat
    z = [jnp.sum(g, axis=0, keepdims=True) for g in (g01[0:4], g01[4:8], g23[0:4], g23[4:8])]
    for a in range(3):
        residual_rows(a, stiff * vs[a][0:1] + z[a + 1] - xs[a][0:1] * z[0])


def stage(coords, force, stiff, near, mask, both_out, stiff_out, near_out, mask_out, sems):
    copies = (
        (coords, both_out.at[0:3]),
        (force, both_out.at[3:6]),
        (stiff, stiff_out),
        (near, near_out),
        (mask, mask_out),
    )
    started = [pltpu.make_async_copy(src, dst, sems.at[k]) for k, (src, dst) in enumerate(copies)]
    for copy in started:
        copy.start()
    for copy in started:
        copy.wait()


def local_first(both, near, mask, weights, field, centre_out, far_side, own_side, feats):
    _, blocks, atoms = both.shape
    slots = near.shape[1]
    first_block = lax.axis_index("space") * blocks
    centre = [jnp.broadcast_to(total(both[a]) * (1.0 / (blocks * atoms)), (8, 128)) for a in range(3)]
    for a in range(3):
        centre_out[8 * a : 8 * a + 8] = centre[a]
    for b in range(blocks):
        xs = centred(read3(both, b), centre)
        put_far_side(far_side, b, xs)
        put_features(feats, b, xs, read3(both, b, 3), True)
        put_own_side(own_side, b, xs, dead_rows(near, mask, b, lambda h: h + first_block, slots))

    def put(b, value):
        field[b] = value

    first_product(weights, far_side, own_side, feats, put, blocks // 2, False)


def get_centre(ref):
    return [ref[8 * a : 8 * a + 8] for a in range(3)]


def order_halo(mate, other, ref):
    odd = lax.rem(lax.axis_index("space"), 2) == 1
    a, b = mate[...], other[...]
    ref[0] = jnp.where(odd, a, b)
    ref[1] = jnp.where(odd, b, a)


def halo(ref, c, blocks):
    return (ref.at[0], c + 1) if c < blocks - 1 else (ref.at[1], c - (blocks - 1))


def halo_first(mate, other, both, stiff, near, mask, centre_in, field_in, weights, selfs, image, sides, far_side, own_side, feats):
    _, blocks, _ = both.shape
    slots = near.shape[1]
    first_block = lax.axis_index("space") * blocks
    centre = get_centre(centre_in)
    base = lambda h: first_block + h + jnp.where(h < blocks - 1, 1 - blocks, 1)
    order_halo(mate, other, sides)
    for c in range(2 * (blocks - 1)):
        ref, k = halo(sides, c, blocks)
        xs = centred(read3(ref, k), centre)
        put_far_side(far_side, c, xs)
        put_features(feats, c, xs, read3(ref, k, 3), True)
    for b in range(blocks):
        xs = centred(read3(both, b), centre)
        put_own_side(own_side, b, xs, dead_rows(near, mask, b, base, slots))

    def put(b, value):
        value = value + field_in[b]
        half = FEATS // 2
        selfs[b] = value[half:]
        xs = centred(read3(both, b), centre)

        def rows(a, row):
            image[a, b : b + 1, :] = row

        apply_local(value[:half], value[half:], xs, read3(both, b, 3), stiff[b : b + 1, :], rows)

    first_product(weights, far_side, own_side, feats, put, blocks // 2, True)


def local_second(both, vector, centre_in, weights, field, feats):
    _, blocks, _ = both.shape
    centre = get_centre(centre_in)
    for b in range(blocks):
        put_features(feats, b, centred(read3(both, b), centre), read3(vector, b), False)

    def put(b, value):
        field[b] = value

    second_product(weights, feats, put, blocks // 2, False)


def total(x):
    return jnp.sum(jnp.sum(x, axis=0, keepdims=True), axis=1, keepdims=True)


def halo_second(vmate, vother, mate, other, both, vector, stiff, centre_in, selfs, field_in, weights, image, sums, sides, vsides, feats):
    _, blocks, _ = both.shape
    centre = get_centre(centre_in)
    order_halo(mate, other, sides)
    order_halo(vmate, vother, vsides)
    for c in range(2 * (blocks - 1)):
        ref, k = halo(sides, c, blocks)
        vref, _ = halo(vsides, c, blocks)
        put_features(feats, c, centred(read3(ref, k), centre), read3(vref, k), False)

    def put(b, value):
        value = value + field_in[b]
        xs = centred(read3(both, b), centre)

        def rows(a, row):
            image[a, b : b + 1, :] = row

        apply_local(value, selfs[b], xs, read3(vector, b), stiff[b : b + 1, :], rows)

    second_product(weights, feats, put, blocks // 2, True)
    f, v, w = both[3:6], vector[...], image[...]
    add = lambda x: total(jnp.sum(x, axis=0))
    s00, s01 = add(f * f), add(f * v)
    shift = s01 / jnp.maximum(s00, 1e-30)
    u = v - shift * f
    w = w - shift * v
    values = [s00, s01, shift, add(f * u), add(u * u), add(f * w + u * v), add(u * w)]
    lane = lax.broadcasted_iota(jnp.int32, sums.shape, 1)
    row = jnp.zeros(sums.shape, F32)
    for k, value in enumerate(values):
        row = jnp.where(lane == k, value, row)
    sums[...] = row


def finish(sums, both, image, image2, solution_out, residual_out, solution_buf, residual_buf, sems):
    table = sums[...]
    s00, s01, shift, s0u, suu, cross, suw = [table[:, k : k + 1] for k in range(7)]
    add = lambda x: jnp.sum(x, axis=0, keepdims=True)
    norm = add(s00)
    alpha = norm / add(s01)
    e = 1.0 - alpha * shift
    norm1 = add(e * e * s00 - 2.0 * alpha * e * s0u + alpha * alpha * suu)
    curve = add(e * e * s01 - alpha * e * cross + alpha * alpha * suw)
    beta = norm1 / norm
    step = norm1 / (curve - beta * norm1 / alpha)
    f, v, w = both[3:6], image[...], image2[...]
    r = f - alpha * v
    solution_buf[...] = alpha * f + step * (r + beta * f)
    residual_buf[...] = r - step * (v - alpha * w + beta * v)
    copies = [
        pltpu.make_async_copy(solution_buf, solution_out, sems.at[0]),
        pltpu.make_async_copy(residual_buf, residual_out, sems.at[1]),
    ]
    for copy in copies:
        copy.start()
    for copy in copies:
        copy.wait()


def call(kernel, outs, args, scratch=(), hbm_in=False, hbm_out=False, sems=0):
    hbm = pl.BlockSpec(memory_space=pltpu.HBM)
    return pl.pallas_call(
        kernel,
        out_shape=[jax.ShapeDtypeStruct(s, d) for s, d in outs],
        in_specs=[hbm if hbm_in else vmem()] * len(args),
        out_specs=[hbm if hbm_out else vmem()] * len(outs),
        scratch_shapes=[pltpu.VMEM(s, d) for s, d in scratch] + ([pltpu.SemaphoreType.DMA((sems,))] if sems else []),
        compiler_params=pltpu.CompilerParams(vmem_limit_bytes=8 * 2 ** 20),
    )(*args)


def per_device(coords, force, restraint, neighbors, mask):
    blocks, parts, atoms = coords.shape
    devices = lax.axis_size("space")
    mates = [(i, i ^ 1) for i in range(devices)]
    others = [pair for i in range(1, devices - 1, 2) for pair in ((i, i + 1), (i + 1, i))]
    flip = lambda x: jnp.transpose(x, (1, 0, 2))
    vec = ((parts, blocks, atoms), F32)
    pair = ((2 * parts, blocks, atoms), F32)
    wshape = ((blocks // 2, blocks // 2, 2 * atoms // 16, 4, 16, atoms), BF16)
    own_scratch = ((blocks, 2 * FEATS, atoms), BF16)
    far = blocks * 2 - 2

    both, stiff, near, live = call(
        stage,
        [pair, (restraint.shape, F32), (neighbors.shape, neighbors.dtype), (mask.shape, mask.dtype)],
        [pltpu.with_memory_space_constraint(x, pltpu.HBM) for x in (flip(coords), flip(force), restraint, neighbors, mask)],
        hbm_in=True,
        sems=5,
    )
    other = lax.ppermute(both, "space", others)
    mate = lax.ppermute(both, "space", mates)
    w1, field, centre = call(
        local_first,
        [wshape, ((blocks, FEATS, atoms), F32), ((24, 128), F32)],
        (both, near, live),
        [((blocks, atoms, atoms), BF16), own_scratch, ((blocks, 3 * FEATS, atoms), BF16)],
    )
    w2, selfs, image = call(
        halo_first,
        [wshape, ((blocks, FEATS // 2, atoms), F32), vec],
        (mate, other, both, stiff, near, live, centre, field),
        [((2,) + pair[0], F32), ((far, atoms, atoms), BF16), own_scratch, ((far, 3 * FEATS, atoms), BF16)],
    )
    vother = lax.ppermute(image, "space", others)
    vmate = lax.ppermute(image, "space", mates)
    (field2,) = call(
        local_second,
        [((blocks, FEATS // 2, atoms), F32)],
        (both, image, centre, w1),
        [((blocks, 3 * FEATS // 2, atoms), BF16)],
    )
    image2, sums = call(
        halo_second,
        [vec, ((devices, 128), F32)],
        (vmate, vother, mate, other, both, image, stiff, centre, selfs, field2, w2),
        [((2,) + pair[0], F32), ((2,) + vec[0], F32), ((far, 3 * FEATS // 2, atoms), BF16)],
    )
    table = lax.all_to_all(sums, "space", 0, 0, tiled=True)
    solved, residual = call(finish, [vec, vec], (table, both, image, image2), [vec, vec], hbm_out=True, sems=2)
    return flip(solved), flip(residual)


def solution(mesh):
    in_specs = (
        P("space", None, None),
        P("space", None, None),
        P("space", None),
        P("space", None),
        P("space", None),
    )
    out_specs = (P("space", None, None), P("space", None, None))
    return jax.shard_map(per_device, mesh=mesh, in_specs=in_specs, out_specs=out_specs, check_vma=False)
```
